32 devices in a mesh: gx: 2 (over core), gy: 4 (over y, x), gz: 4 (over z).
Axes of the slice: x: 2, y: 2, z: 4, core: 2. Of those that a mesh axis runs over, the one named last changes fastest.
Arguments:
- pressure_rhs: float32 [32, 128, 2048], P('gx', 'gy', 'gz'), may hold values from -6 to 6
- shift_diag: float32 [32, 128, 2048], P('gx', 'gy', 'gz'), may hold values from 0.02 to 0.3
- positions: float32 [3, 262144], P(None, ('gx', 'gy', 'gz')), may hold values from -6 to 6
- normals: float32 [3, 262144], P(None, ('gx', 'gy', 'gz')), may hold values from -6 to 6
- tension: float32 [262144], P(('gx', 'gy', 'gz')), may hold values from 0.3 to 3
- edge_weight: float32 [6, 262144], P(None, ('gx', 'gy', 'gz')), may hold values from 0.5 to 2
- owner_map: int32 [262144, 1], P(('gx', 'gy', 'gz')), may hold values from 0 to 31; in each aligned block of 8192 rows (0 to 8191, 8192 to 16383, ...) at most 1024 rows name the same one
- cell_map: int32 [262144], P(('gx', 'gy', 'gz')), may hold values from 0 to 262143
- connectivity: int32 [6, 262144], P(None, ('gx', 'gy', 'gz')), may hold values from 0 to 262143, as said below
Outputs:
- pressure: float32 [32, 128, 2048], P('gx', 'gy', 'gz')
- surface_force: float32 [3, 262144], P(None, ('gx', 'gy', 'gz'))
The draws below stay inside these ranges and needn't reach their ends.
Inputs may be any that keep to these rules, and one draw needn't show every extreme that they name: `connectivity`: each neighbour index differs from the point's own index by 1 to 64, counted cyclically over 262144; the distance 64 occurs. `owner_map`: among the points of one device no owner is named more than 1024 times, a bound that some block reaches.
All inputs are finite; a program needn't handle non-finite values.
Results may differ from the reference program's by a relative error of at most 0.0003.
Values sent between devices are 32-bit elements; how exact they have to be, the bound alone decides.
A program may use at most 192 MiB of HBM per device.

```python
import math
import jax
import jax.numpy as jnp
import numpy as np

CX = 16
CY = 32
CZ = 512
PTS_DEV = 8192
NEIGH = 6
HALO = 64
SMOOTH = 3
COARSE_SMOOTH = 4
POINTS = 262144
CAP = 1024
NX = 32
NY = 128
NZ = 2048
N_GY = 4
N_GZ = 4
DEVICES = 32


def draw_connectivity(key, part):
    first = jax.random.fold_in(key, 11)
    second = jax.random.fold_in(key, 12)
    reach = jax.random.randint(first, (NEIGH, POINTS), 1, HALO + 1)
    reach = reach.at[0, 0].set(HALO)
    sign = jax.random.randint(second, (NEIGH, POINTS), 0, 2) * 2 - 1
    base = jnp.arange(POINTS, dtype=jnp.int32)[None, :]
    return ((base + sign * reach) % POINTS).astype(jnp.int32)


def plant(entries, stream_key, smallest, high):
    dims = entries.shape
    place = [jax.random.randint(jax.random.fold_in(stream_key, axis), (), 0, dims[axis]) for axis in range(len(dims))]
    entries = entries.at[tuple(place)].set(smallest)
    longest = dims.index(max(dims))
    place[longest] = (place[longest] + 1) % dims[longest]
    return entries.at[tuple(place)].set(high)


def block_levels(own_key, extent, pieces, least, top_value):
    factor_of, own = 1.0, jax.random.fold_in(own_key, 6)
    for axis_at, shards_of in pieces:
        heights = jnp.exp(jax.random.uniform(jax.random.fold_in(own, axis_at), (shards_of,), jnp.float32, least / len(pieces), top_value / len(pieces)))
        factor_of = factor_of * jnp.repeat(heights, extent[axis_at] // shards_of).reshape([-1 if axis == axis_at else 1 for axis in range(len(extent))])
    return factor_of


def deal_out(key, own, number, rows, amount, top, most, slope):
    sequence = jax.random.permutation(key, amount)
    heavy_load, common = shares(amount, rows * top, most, slope, True), shares(amount, rows * top, most, slope, False)
    places = jnp.arange(amount)

    def named(tallies, rotation):
        used = int((tallies > 0).sum())
        fixed = max(1, used // 4)
        shifted = fixed + (places - fixed + rotation * (used - fixed)) % max(1, amount - fixed)
        return jnp.zeros((amount,), jnp.int32).at[sequence[jnp.where(places < fixed, places, shifted)]].set(jnp.asarray(tallies, jnp.int32))

    tallies = jnp.where(number % 4 == 0, named(heavy_load, number // 4), named(common, number - number // 4 - 1))
    mixed = jax.random.permutation(jax.random.fold_in(own, 3), amount)
    giver, taker = mixed[0:amount // 2 * 2:2], mixed[1:amount // 2 * 2:2]
    room = jnp.minimum(tallies[giver] - 1, most - tallies[taker]) // 2
    room = jnp.where((giver == sequence[0]) | (taker == sequence[0]) | (tallies[taker] == 0), 0, jnp.maximum(room, 0))
    shifted = jax.random.randint(jax.random.fold_in(own, 4), (amount // 2,), 0, 1 << 20) % (room + 1)
    tallies = tallies.at[giver].add(-shifted).at[taker].add(shifted)
    members = jnp.searchsorted(jnp.cumsum(tallies), jnp.arange(rows * top), side="right").astype(jnp.int32)
    listing = members.reshape(top, rows).T
    listing = listing[jax.random.permutation(jax.random.fold_in(own, 1), rows)]
    rotation = jax.random.randint(jax.random.fold_in(own, 2), (rows, 1), 0, top)
    return jnp.take_along_axis(listing, (jnp.arange(top)[None, :] + rotation) % top, axis=1)


def shares(count, total, bound, slope, full):
    weights = [(1 << 20) // math.isqrt(grade ** slope) + 1 for grade in range(1, count + 1)]
    largest = bound if full else min(bound, max(-(-total // count), total * weights[0] // sum(weights)))
    least = 1 if total - largest >= count - 1 else 0
    given, surplus = [largest] + [least] * (count - 1), total - largest - least * (count - 1)
    while surplus > 0:
        free = [i for i in range(1, count) if given[i] < largest] or [i for i in range(1, count) if given[i] < bound]
        whole, budget = sum([weights[i] for i in free]), surplus
        for i in free:
            more = min(bound - given[i], max(1, budget * weights[i] // whole), surplus)
            given[i] = given[i] + more
            surplus = surplus - more
    return np.array(given)


def scatter_about(stream_key, extent, scale, most, split=(), kind=jnp.bfloat16):
    gain = block_levels(stream_key, extent, split, -0.22, 0.18) if split else 1.0
    array = jax.random.normal(stream_key, extent, jnp.float32) * scale * gain
    return jnp.minimum(jnp.maximum(array, -most), most).astype(kind)


def setup_inputs(seed: int = 0) -> dict:
    keys = jax.random.split(jax.random.key(seed), 10)
    pressure_rhs = scatter_about(keys[0], (NX, NY, NZ), 1.0, 6.0, ((0, 2), (1, 4), (2, 4)), jnp.float32)
    shift_diag = jnp.clip(jnp.exp(math.log(0.3) - 2.7080503 * jax.random.uniform(keys[1], (NX, NY, NZ), jnp.float32) ** block_levels(keys[1], (NX, NY, NZ), ((0, 2), (1, 4), (2, 4)), -0.2, 0.2)), 0.02, 0.3)
    positions = scatter_about(keys[2], (3, POINTS), 1.0, 6.0, ((1, 32),), jnp.float32)
    normals = scatter_about(keys[3], (3, POINTS), 1.0, 6.0, ((1, 32),), jnp.float32)
    tension = jnp.clip(jnp.exp(math.log(3.0) - 2.3025851 * jax.random.uniform(keys[4], (POINTS,), jnp.float32) ** block_levels(keys[4], (POINTS,), ((0, 32),), -0.2, 0.2)), 0.3, 3.0)
    edge_weight = jnp.clip(jnp.exp(math.log(2.0) - 1.3862944 * jax.random.uniform(keys[5], (NEIGH, POINTS), jnp.float32) ** block_levels(keys[5], (NEIGH, POINTS), ((1, 32),), -0.2, 0.2)), 0.5, 2.0)
    owner_map_keys = jax.random.split(jax.random.fold_in(keys[6], 1), POINTS // PTS_DEV)
    owner_map_turns = jax.random.permutation(jax.random.fold_in(keys[6], 3), POINTS // PTS_DEV)
    owner_map = jax.vmap(lambda own, number: deal_out(jax.random.fold_in(keys[6], 2), own, number, PTS_DEV, DEVICES, 1, CAP, 2))(owner_map_keys, owner_map_turns).reshape((POINTS, 1))
    cell_map = plant(jax.random.randint(keys[7], (POINTS,), 0, CX * CY * CZ), jax.random.fold_in(keys[7], 1), 0, (CX * CY * CZ) - 1).astype(jnp.int32)
    connectivity = draw_connectivity(jax.random.fold_in(keys[9], 71), 0)
    return dict(pressure_rhs=pressure_rhs, shift_diag=shift_diag, positions=positions, normals=normals, tension=tension, edge_weight=edge_weight, owner_map=owner_map, cell_map=cell_map, connectivity=connectivity)


centre = 1.125
spread = 0.875


def operate(field, shift):
    padded = jnp.pad(field, 1)
    beside = padded[2:, 1:-1, 1:-1] + padded[:-2, 1:-1, 1:-1]
    beside = beside + padded[1:-1, 2:, 1:-1] + padded[1:-1, :-2, 1:-1]
    beside = beside + padded[1:-1, 1:-1, 2:] + padded[1:-1, 1:-1, :-2]
    return (6.0 + shift) * field - beside


def chebyshev(target, shift, start, sweeps):
    inverse = 1.0 / (6.0 + shift)
    ratio = centre / spread
    factor = 1.0 / ratio
    if start is None:
        update = inverse * target / centre
        answer = update
    else:
        update = inverse * (target - operate(start, shift)) / centre
        answer = start + update
    for sweep in range(1, sweeps):
        remain = inverse * (target - operate(answer, shift))
        factor_new = 1.0 / (2.0 * ratio - factor)
        update = factor_new * factor * update + (2.0 * factor_new / spread) * remain
        answer = answer + update
        factor = factor_new
    return answer


def blocks(field):
    nxh, nyh, nzh = field.shape[0] // 2, field.shape[1] // 2, field.shape[2] // 2
    return field.reshape(nxh, 2, nyh, 2, nzh, 2)


def reference(pressure_rhs, shift_diag, positions, normals, tension, edge_weight, owner_map, cell_map, connectivity):
    neighbours = positions[:, connectivity]
    surface_force = tension[None, :] * jnp.sum(edge_weight[None, :, :] * (neighbours - positions[:, None, :]), axis=1)
    jump = jnp.sum(surface_force * normals, axis=0)
    owner = owner_map[:, 0]
    ox = owner // (N_GY * N_GZ)
    oy = (owner // N_GZ) % N_GY
    oz = owner % N_GZ
    cx = cell_map // (CY * CZ)
    cy = (cell_map // CZ) % CY
    cz = cell_map % CZ
    forcing = pressure_rhs.at[ox * CX + cx, oy * CY + cy, oz * CZ + cz].add(jump)
    smooth = chebyshev(forcing, shift_diag, None, SMOOTH)
    remain = forcing - operate(smooth, shift_diag)
    coarse_rhs = 0.5 * jnp.sum(blocks(remain), axis=(1, 3, 5))
    coarse_shift = 4.0 * jnp.mean(blocks(shift_diag), axis=(1, 3, 5))
    coarse_fix = chebyshev(coarse_rhs, coarse_shift, None, COARSE_SMOOTH)
    spreadout = jnp.repeat(jnp.repeat(jnp.repeat(coarse_fix, 2, axis=0), 2, axis=1), 2, axis=2)
    pressure = chebyshev(forcing, shift_diag, smooth + spreadout, SMOOTH)
    return pressure, surface_force
```

```python
import functools

import jax
import jax.numpy as jnp
from jax import lax
from jax.experimental import pallas as pl
from jax.experimental.pallas import tpu as pltpu
from jax.sharding import PartitionSpec as P

HALO = 64
SMOOTH = 3
COARSE_SMOOTH = 4


centre = 1.125
spread = 0.875


def padded_2(cells, sides, width, closed):
    for axis, dim in sides:
        count = lax.axis_size(axis)
        ends = count if closed else count - 1
        head = lax.slice_in_dim(cells, 0, width, axis=dim)
        tail = lax.slice_in_dim(cells, cells.shape[dim] - width, cells.shape[dim], axis=dim)
        cells = jnp.concatenate(
            [
                lax.ppermute(tail, axis, [(i, (i + 1) % count) for i in range(ends)]),
                cells,
                lax.ppermute(head, axis, [((i + 1) % count, i) for i in range(ends)]),
            ],
            axis=dim,
        )
    return cells


def stencil(padded, field, shift):
    beside = padded[2:, 1:-1, 1:-1] + padded[:-2, 1:-1, 1:-1]
    beside = beside + padded[1:-1, 2:, 1:-1] + padded[1:-1, :-2, 1:-1]
    beside = beside + padded[1:-1, 1:-1, 2:] + padded[1:-1, 1:-1, :-2]
    return (6.0 + shift) * field - beside


def local_apply(field, shift):
    return stencil(jnp.pad(field, 1), field, shift)


def chebyshev(target, shift, start, sweeps, apply_fn, inside):
    inverse = 1.0 / (6.0 + shift)
    ratio = centre / spread
    factor = 1.0 / ratio
    if start is None:
        update = inverse * target / centre
        answer = update
    else:
        update = inverse * (target - apply_fn(start, shift)) / centre
        update = update * inside
        answer = start + update
    for sweep in range(1, sweeps):
        remain = inverse * (target - apply_fn(answer, shift))
        if inside is not None:
            remain = remain * inside
        factor_new = 1.0 / (2.0 * ratio - factor)
        update = factor_new * factor * update + 2.0 * factor_new / spread * remain
        answer = answer + update
        factor = factor_new
    return answer


def domain_mask(shape, width):
    places = (lax.axis_index("gx"), lax.axis_index("gy"), lax.axis_index("gz"))
    counts = (lax.axis_size("gx"), lax.axis_size("gy"), lax.axis_size("gz"))
    factors = []
    for which in range(3):
        length = shape[which]
        where = places[which] * length - width + jnp.arange(length + 2 * width, dtype=jnp.int32)
        factors.append(((where >= 0) & (where < length * counts[which])).astype(jnp.float32))
    return factors[0][:, None, None] * factors[1][None, :, None] * factors[2][None, None, :]


def interior(field, width):
    return field[width:-width, width:-width, width:-width]


LANES = 2 * HALO
HIGH = lax.Precision.HIGHEST


def pair_matrix(rows, cols, offset=0):
    r = lax.broadcasted_iota(jnp.int32, (rows, cols), 0)
    c = lax.broadcasted_iota(jnp.int32, (rows, cols), 1)
    return (r == (c + offset) // 2).astype(jnp.float32)


def pool(field):
    nx, ny, nz = field.shape
    halves = jnp.sum(field.reshape(nx // 2, 2, ny, nz), axis=1)
    flat = halves.reshape(nx // 2 * ny, nz)
    along_z = jnp.dot(flat, pair_matrix(nz // 2, nz).T, precision=HIGH)
    along_y = jnp.dot(
        pair_matrix(nx // 2 * ny // 2, nx // 2 * ny), along_z, precision=HIGH
    )
    return along_y.reshape(nx // 2, ny // 2, nz // 2)


def spread_out(coarse, crop):
    nx, ny, nz = coarse.shape
    along_z = jnp.dot(
        coarse.reshape(nx * ny, nz), pair_matrix(nz, 2 * nz - 2 * crop, crop), precision=HIGH
    ).reshape(nx, ny, 2 * nz - 2 * crop)
    fan = jnp.broadcast_to(
        pair_matrix(ny, 2 * ny - 2 * crop, crop).T[None], (nx, 2 * ny - 2 * crop, ny)
    )
    along_y = jnp.einsum("xyb,xbc->xyc", fan, along_z, precision=HIGH)
    twice = jnp.broadcast_to(along_y[:, None], (nx, 2) + along_y.shape[1:])
    twice = twice.reshape((2 * nx,) + along_y.shape[1:])
    return twice[crop : 2 * nx - crop]


def split3(x):
    a = x.astype(jnp.bfloat16)
    rest = x - a.astype(jnp.float32)
    b = rest.astype(jnp.bfloat16)
    c = (rest - b.astype(jnp.float32)).astype(jnp.bfloat16)
    return a, b, c


def points_kernel(
    ndevice, capacity, pos_ref, nrm_ref, ten_ref, wgt_ref, con_ref, own_ref, cel_ref,
    force_ref, packed_ref, carry_ref,
):
    step = pl.program_id(0)
    chunk = ten_ref.shape[1]

    @pl.when(step == 0)
    def _():
        packed_ref[...] = jnp.zeros_like(packed_ref)
        carry_ref[...] = jnp.zeros_like(carry_ref)

    jumps = []
    for sub in range(chunk // LANES):
        here = pl.ds(sub * LANES, LANES)
        base = pl.multiple_of(step * chunk + sub * LANES, LANES)
        lower = pos_ref[:, pl.ds(base, LANES)]
        upper = pos_ref[:, pl.ds(base + LANES, LANES)]
        centre_pos = jnp.concatenate([lower[:, HALO:], upper[:, :HALO]], axis=1)
        total = jnp.zeros_like(lower)
        for which in range(con_ref.shape[0]):
            index = con_ref[which : which + 1, here] - base
            wide = jnp.broadcast_to(index, lower.shape)
            low = jnp.bitwise_and(wide, LANES - 1)
            near = jnp.take_along_axis(lower, low, axis=1, mode="promise_in_bounds")
            far = jnp.take_along_axis(upper, low, axis=1, mode="promise_in_bounds")
            picked = jnp.where(wide < LANES, near, far)
            total = total + wgt_ref[which : which + 1, here] * (picked - centre_pos)
        force = ten_ref[:, here] * total[:3]
        force_ref[:, here] = force
        jumps.append(jnp.sum(force * nrm_ref[:, here], axis=0, keepdims=True))
    jump = jnp.concatenate(jumps, axis=1)

    hot = (lax.broadcasted_iota(jnp.int32, (ndevice, chunk), 0) == own_ref[...]).astype(jnp.float32)
    hot_half = hot.astype(jnp.bfloat16)
    before = (
        lax.broadcasted_iota(jnp.int32, (chunk, chunk), 0)
        < lax.broadcasted_iota(jnp.int32, (chunk, chunk), 1)
    ).astype(jnp.bfloat16)
    earlier = jnp.dot(hot_half, before, preferred_element_type=jnp.float32) + carry_ref[...]
    rank = jnp.sum(hot * earlier, axis=0, keepdims=True).astype(jnp.int32)
    carry_ref[...] = carry_ref[...] + jnp.sum(hot, axis=1, keepdims=True)
    slots = (
        lax.broadcasted_iota(jnp.int32, (capacity, chunk), 0) == rank
    ).astype(jnp.float32).astype(jnp.bfloat16)
    cell = cel_ref[...]
    parts = [piece.astype(jnp.float32) for piece in split3(jump)]
    for bits in (0, 8, 16):
        piece = jnp.bitwise_and(jnp.right_shift(cell, bits), 255).astype(jnp.float32)
        parts.append(piece)
    left = jnp.concatenate([(hot * part).astype(jnp.bfloat16) for part in parts], axis=0)
    packed = lax.dot_general(
        left, slots, (((1,), (1,)), ((), ())), preferred_element_type=jnp.float32
    )
    n = ndevice
    values = packed[0:n] + packed[n : 2 * n] + packed[2 * n : 3 * n]
    cells = packed[3 * n : 4 * n] + 256.0 * packed[4 * n : 5 * n] + 65536.0 * packed[5 * n :]
    packed_ref[:, :capacity] += values
    packed_ref[:, capacity:] += cells


def points(padded, normals, tension, edge_weight, relative, owner_ids, cell_map, ndevice, capacity):
    npoint = tension.shape[0]
    chunk = 4 * LANES if npoint % (4 * LANES) == 0 else LANES
    padded = jnp.concatenate([padded, jnp.zeros((5, padded.shape[1]), jnp.float32)], axis=0)
    neigh = relative.shape[0]

    def rows(count):
        return pl.BlockSpec((count, chunk), lambda i: (0, i))

    return pl.pallas_call(
        functools.partial(points_kernel, ndevice, capacity),
        grid=(npoint // chunk,),
        in_specs=[
            pl.BlockSpec(padded.shape, lambda i: (0, 0)),
            rows(3), rows(1), rows(neigh), rows(neigh), rows(1), rows(1),
        ],
        out_specs=[rows(3), pl.BlockSpec((ndevice, 2 * capacity), lambda i: (0, 0))],
        out_shape=[
            jax.ShapeDtypeStruct((3, npoint), jnp.float32),
            jax.ShapeDtypeStruct((ndevice, 2 * capacity), jnp.float32),
        ],
        scratch_shapes=[pltpu.VMEM((ndevice, 1), jnp.float32)],
        cost_estimate=pl.CostEstimate(
            flops=2 * npoint * capacity * 6 * ndevice, bytes_accessed=40000000, transcendentals=0
        ),
    )(
        padded, normals, tension[None], edge_weight, relative, owner_ids[None], cell_map[None]
    )


def scatter_kernel(rhs_ref, val_ref, row_ref, col_ref, out_ref):
    @pl.when(pl.program_id(0) == 0)
    def _():
        out_ref[...] = rhs_ref[...]

    nrow, ncol = out_ref.shape
    count = val_ref.shape[2]
    value = val_ref[0]
    first = value.astype(jnp.bfloat16)
    second = (value - first.astype(jnp.float32)).astype(jnp.bfloat16)
    by_row = (
        (lax.broadcasted_iota(jnp.int32, (nrow, count), 0) == row_ref[0])
        .astype(jnp.float32)
        .astype(jnp.bfloat16)
    )
    same = lax.broadcasted_iota(jnp.int32, (ncol, count), 0) == col_ref[0]
    total = out_ref[...]
    for piece in (first, second):
        by_col = jnp.where(same, piece.astype(jnp.float32), 0.0).astype(jnp.bfloat16)
        total = total + lax.dot_general(
            by_row, by_col, (((1,), (1,)), ((), ())), preferred_element_type=jnp.float32
        )
    out_ref[...] = total


def scatter(rhs, values, cells):
    nx, ny, nz = rhs.shape
    nrow = nx * ny
    sources, count = values.shape
    rows = cells // nz
    cols = cells - rows * nz
    one = pl.BlockSpec((1, 1, count), lambda i: (i, 0, 0))
    whole = pl.BlockSpec((nrow, nz), lambda i: (0, 0))
    out = pl.pallas_call(
        scatter_kernel,
        grid=(sources,),
        in_specs=[whole, one, one, one],
        out_specs=whole,
        out_shape=jax.ShapeDtypeStruct((nrow, nz), jnp.float32),
        cost_estimate=pl.CostEstimate(
            flops=4 * nrow * nz * sources * count, bytes_accessed=4000000, transcendentals=0
        ),
    )(rhs.reshape(nrow, nz), values[:, None], rows[:, None], cols[:, None])
    return out.reshape(nx, ny, nz)


def body(
    pressure_rhs,
    shift_diag,
    positions,
    normals,
    tension,
    edge_weight,
    owner_map,
    cell_map,
    connectivity,
):
    npoint = positions.shape[1]
    ndevice = lax.axis_size(("gx", "gy", "gz"))
    total = npoint * ndevice
    begin = lax.axis_index(("gx", "gy", "gz")) * npoint
    padded = padded_2(positions, ((("gx", "gy", "gz"), 1),), HALO, True)
    relative = (connectivity - begin + HALO + total) % total
    capacity = 4 * npoint // ndevice
    surface_force, packed = points(
        padded, normals, tension, edge_weight, relative, owner_map[:, 0], cell_map,
        ndevice, capacity,
    )
    got = lax.all_to_all(packed, ("gx", "gy", "gz"), split_axis=0, concat_axis=0, tiled=True)
    forcing = scatter(pressure_rhs, got[:, :capacity], got[:, capacity:].astype(jnp.int32))

    sides = (("gx", 0), ("gy", 1), ("gz", 2))
    shape = pressure_rhs.shape
    coarse_shift = 0.5 * pool(shift_diag)
    last = SMOOTH
    width = SMOOTH + SMOOTH - 1
    reach = (last + 1) // 2
    coarse_width = COARSE_SMOOTH - 1 + reach
    shift_wide = padded_2(shift_diag, sides, width, False)
    forcing_wide = padded_2(forcing, sides, width, False)
    smooth_wide = chebyshev(
        forcing_wide, shift_wide, None, SMOOTH, local_apply, domain_mask(shape, width)
    )
    near = slice(width - 1, -(width - 1))
    near = (near, near, near)
    remain = interior(forcing_wide, width) - stencil(
        smooth_wide[near], interior(smooth_wide, width), interior(shift_wide, width)
    )
    coarse_rhs = 0.5 * pool(remain)
    coarse_sides = (("gx", 1), ("gy", 2), ("gz", 3))
    coarse_wide = padded_2(
        jnp.stack([coarse_rhs, coarse_shift]), coarse_sides, coarse_width, False
    )
    coarse_fix = chebyshev(
        coarse_wide[0], coarse_wide[1], None, COARSE_SMOOTH, local_apply,
        domain_mask(coarse_rhs.shape, coarse_width),
    )
    coarse_fix = interior(coarse_fix, coarse_width - reach)
    spreadout = spread_out(coarse_fix, 2 * reach - last)
    trim = width - last
    start_wide = interior(smooth_wide, trim) + spreadout
    pressure = interior(
        chebyshev(
            interior(forcing_wide, trim), interior(shift_wide, trim), start_wide, SMOOTH,
            local_apply, domain_mask(shape, last),
        ),
        last,
    )
    return (pressure, surface_force)


def solution(mesh):
    return jax.shard_map(
        body,
        mesh=mesh,
        in_specs=(
            P("gx", "gy", "gz"),
            P("gx", "gy", "gz"),
            P(None, ("gx", "gy", "gz")),
            P(None, ("gx", "gy", "gz")),
            P(("gx", "gy", "gz")),
            P(None, ("gx", "gy", "gz")),
            P(("gx", "gy", "gz"), None),
            P(("gx", "gy", "gz")),
            P(None, ("gx", "gy", "gz")),
        ),
        out_specs=(P("gx", "gy", "gz"), P(None, ("gx", "gy", "gz"))),
        check_vma=False,
    )
```

```python
import functools

import jax
import jax.numpy as jnp
from jax import lax
from jax.experimental import pallas as pl
from jax.experimental.pallas import tpu as pltpu
from jax.sharding import PartitionSpec as P

HALO = 64
SMOOTH = 3
COARSE_SMOOTH = 4


centre = 1.125
spread = 0.875


def padded_2(cells, sides, closed):
    for axis, dim, width in sides:
        count = lax.axis_size(axis)
        ends = count if closed else count - 1
        head = lax.slice_in_dim(cells, 0, width, axis=dim)
        tail = lax.slice_in_dim(cells, cells.shape[dim] - width, cells.shape[dim], axis=dim)
        cells = jnp.concatenate(
            [
                lax.ppermute(tail, axis, [(i, (i + 1) % count) for i in range(ends)]),
                cells,
                lax.ppermute(head, axis, [((i + 1) % count, i) for i in range(ends)]),
            ],
            axis=dim,
        )
    return cells


def factors(sweeps):
    ratio = centre / spread
    fac = 1.0 / ratio
    pairs = [(0.0, 1.0 / centre)]
    for _ in range(1, sweeps):
        fac_new = 1.0 / (2.0 * ratio - fac)
        pairs.append((fac_new * fac, 2.0 * fac_new / spread))
        fac = fac_new
    return pairs


def beside(ref, x, cells):
    ny, nz = cells.shape
    total = ref[x - 1] + ref[x + 1]
    total = total + pltpu.roll(cells, 1, 0) + pltpu.roll(cells, ny - 1, 0)
    return total + pltpu.roll(cells, 1, 1) + pltpu.roll(cells, nz - 1, 1)


def sweep(rhs, inverse, src, dst, update, first, last, pair, keep=None):
    old, new = pair

    def slab(x, carry):
        cells = src[x]
        change = new * (inverse[x] * (rhs[x] + beside(src, x, cells)) - cells)
        if old:
            change = change + old * update[x]
        if keep is None:
            update[x] = change
            dst[x] = cells + change
        else:
            keep(x, cells + change)
        return carry

    lax.fori_loop(first, last, slab, 0)


def begin(rhs, inverse, dst, update, slabs):
    def slab(x, carry):
        change = inverse[x] * rhs[x] * (1.0 / centre)
        update[x] = change
        dst[x] = change
        return carry

    lax.fori_loop(0, slabs, slab, 0)


def down_kernel(wx, wy, wz, rhs, inverse, shift, smooth, remain, one, update):
    slabs = rhs.shape[0]
    ny, nz = remain.shape[1:]
    pairs = factors(SMOOTH)
    bufs = (one, smooth) if SMOOTH % 2 == 0 else (smooth, one)
    begin(rhs, inverse, bufs[0], update, slabs)
    for k in range(1, SMOOTH):
        sweep(
            rhs, inverse, bufs[(k - 1) % 2], bufs[k % 2], update, k, slabs - k, pairs[k]
        )

    def slab(x, carry):
        cells = smooth[x]
        near = rhs[x] + beside(smooth, x, cells)
        core = (slice(wy, wy + ny), slice(wz, wz + nz))
        remain[x - wx] = near[core] - (6.0 + shift[x - wx]) * cells[core]
        return carry

    lax.fori_loop(wx, slabs - wx, slab, 0)


def up_kernel(
    wx, wy, wz, cx, coarse, rhs, inverse, smooth, pressure,
    fix_a, fix_b, fix_update, one, two, update,
):
    crhs, cinverse = coarse.at[0], coarse.at[1]
    cslabs, cny, cnz = fix_a.shape
    slabs, fny, fnz = one.shape
    ny, nz = pressure.shape[1:]
    pairs = factors(COARSE_SMOOTH)
    bufs = (fix_a, fix_b)
    begin(crhs, cinverse, fix_a, fix_update, cslabs)
    for k in range(1, COARSE_SMOOTH):
        sweep(
            crhs, cinverse, bufs[(k - 1) % 2], bufs[k % 2], fix_update, k, cslabs - k, pairs[k]
        )
    fix = bufs[(COARSE_SMOOTH - 1) % 2]

    low = cx - (SMOOTH + 1) // 2
    count = cslabs - 2 * low
    flat = fix[low : low + count].reshape(count * cny, cnz)

    def onehot(shape, offset_f, offset_c, fine_dim, fine_per, coarse_per):
        f = lax.broadcasted_iota(jnp.int32, shape, fine_dim)
        c = lax.broadcasted_iota(jnp.int32, shape, 1 - fine_dim)
        block, inner = 0, f
        for g in range(1, shape[fine_dim] // fine_per):
            block = block + (f >= g * fine_per).astype(jnp.int32)
        inner = f - block * fine_per
        half = jnp.right_shift(inner - offset_f + 2 * offset_c, 1)
        return (c == half + block * coarse_per).astype(jnp.float32).astype(jnp.bfloat16)

    fan_y = onehot((count * fny, count * cny), wy, wy, 0, fny, cny)
    fan_z = onehot((cnz, fnz), wz, wz, 1, fnz, cnz)
    tall = sum(
        jnp.dot(fan_y, piece, preferred_element_type=jnp.float32) for piece in split3(flat)
    )
    full = sum(
        jnp.dot(piece, fan_z, preferred_element_type=jnp.float32) for piece in split3(tall)
    )
    for j in range(count):
        part = full[j * fny : (j + 1) * fny]
        for half in range(2):
            x = wx + 2 * (low + j - cx) + half
            if wx - SMOOTH <= x < slabs - wx + SMOOTH:
                one[x] = smooth[x] + part

    pairs = factors(SMOOTH)
    bufs = (one, two)

    def keep(x, cells):
        pressure[x - wx] = cells[wy : wy + ny, wz : wz + nz]

    edge = wx - SMOOTH
    for k in range(SMOOTH):
        sweep(
            rhs, inverse, bufs[k % 2], bufs[(k + 1) % 2], update,
            edge + k + 1, slabs - edge - k - 1, pairs[k], keep if k == SMOOTH - 1 else None,
        )


LANES = 2 * HALO
HIGH = lax.Precision.HIGHEST


def pair_matrix(rows, cols, offset=0):
    r = lax.broadcasted_iota(jnp.int32, (rows, cols), 0)
    c = lax.broadcasted_iota(jnp.int32, (rows, cols), 1)
    return (r == (c + offset) // 2).astype(jnp.float32)


def pool(field):
    nx, ny, nz = field.shape
    halves = jnp.sum(field.reshape(nx // 2, 2, ny, nz), axis=1)
    flat = halves.reshape(nx // 2 * ny, nz)
    along_z = jnp.dot(flat, pair_matrix(nz // 2, nz).T, precision=HIGH)
    along_y = jnp.dot(
        pair_matrix(nx // 2 * ny // 2, nx // 2 * ny), along_z, precision=HIGH
    )
    return along_y.reshape(nx // 2, ny // 2, nz // 2)


def split3(x):
    a = x.astype(jnp.bfloat16)
    rest = x - a.astype(jnp.float32)
    b = rest.astype(jnp.bfloat16)
    c = (rest - b.astype(jnp.float32)).astype(jnp.bfloat16)
    return a, b, c


def points_kernel(
    ndevice, capacity, pos_ref, nrm_ref, ten_ref, wgt_ref, con_ref, own_ref, cel_ref,
    force_ref, packed_ref, carry_ref,
):
    step = pl.program_id(0)
    chunk = ten_ref.shape[1]

    @pl.when(step == 0)
    def _():
        packed_ref[...] = jnp.zeros_like(packed_ref)
        carry_ref[...] = jnp.zeros_like(carry_ref)

    jumps = []
    for sub in range(chunk // LANES):
        here = pl.ds(sub * LANES, LANES)
        base = pl.multiple_of(step * chunk + sub * LANES, LANES)
        lower = pos_ref[:, pl.ds(base, LANES)]
        upper = pos_ref[:, pl.ds(base + LANES, LANES)]
        centre_pos = jnp.concatenate([lower[:, HALO:], upper[:, :HALO]], axis=1)
        total = jnp.zeros_like(lower)
        for which in range(con_ref.shape[0]):
            index = con_ref[which : which + 1, here] - base
            wide = jnp.broadcast_to(index, lower.shape)
            low = jnp.bitwise_and(wide, LANES - 1)
            near = jnp.take_along_axis(lower, low, axis=1, mode="promise_in_bounds")
            far = jnp.take_along_axis(upper, low, axis=1, mode="promise_in_bounds")
            picked = jnp.where(wide < LANES, near, far)
            total = total + wgt_ref[which : which + 1, here] * (picked - centre_pos)
        force = ten_ref[:, here] * total[:3]
        force_ref[:, here] = force
        jumps.append(jnp.sum(force * nrm_ref[:, here], axis=0, keepdims=True))
    jump = jnp.concatenate(jumps, axis=1)

    hot = (lax.broadcasted_iota(jnp.int32, (ndevice, chunk), 0) == own_ref[...]).astype(jnp.float32)
    hot_half = hot.astype(jnp.bfloat16)
    before = (
        lax.broadcasted_iota(jnp.int32, (chunk, chunk), 0)
        < lax.broadcasted_iota(jnp.int32, (chunk, chunk), 1)
    ).astype(jnp.bfloat16)
    earlier = jnp.dot(hot_half, before, preferred_element_type=jnp.float32) + carry_ref[...]
    rank = jnp.sum(hot * earlier, axis=0, keepdims=True).astype(jnp.int32)
    carry_ref[...] = carry_ref[...] + jnp.sum(hot, axis=1, keepdims=True)
    slots = (
        lax.broadcasted_iota(jnp.int32, (capacity, chunk), 0) == rank
    ).astype(jnp.float32).astype(jnp.bfloat16)
    cell = cel_ref[...]
    parts = [piece.astype(jnp.float32) for piece in split3(jump)]
    for bits in (0, 8, 16):
        piece = jnp.bitwise_and(jnp.right_shift(cell, bits), 255).astype(jnp.float32)
        parts.append(piece)
    left = jnp.concatenate([(hot * part).astype(jnp.bfloat16) for part in parts], axis=0)
    packed = lax.dot_general(
        left, slots, (((1,), (1,)), ((), ())), preferred_element_type=jnp.float32
    )
    n = ndevice
    values = packed[0:n] + packed[n : 2 * n] + packed[2 * n : 3 * n]
    cells = packed[3 * n : 4 * n] + 256.0 * packed[4 * n : 5 * n] + 65536.0 * packed[5 * n :]
    packed_ref[:, :capacity] += values
    packed_ref[:, capacity:] += cells


def points(padded, normals, tension, edge_weight, relative, owner_ids, cell_map, ndevice, capacity):
    npoint = tension.shape[0]
    chunk = 4 * LANES if npoint % (4 * LANES) == 0 else LANES
    padded = jnp.concatenate([padded, jnp.zeros((5, padded.shape[1]), jnp.float32)], axis=0)
    neigh = relative.shape[0]

    def rows(count):
        return pl.BlockSpec((count, chunk), lambda i: (0, i))

    return pl.pallas_call(
        functools.partial(points_kernel, ndevice, capacity),
        grid=(npoint // chunk,),
        in_specs=[
            pl.BlockSpec(padded.shape, lambda i: (0, 0)),
            rows(3), rows(1), rows(neigh), rows(neigh), rows(1), rows(1),
        ],
        out_specs=[rows(3), pl.BlockSpec((ndevice, 2 * capacity), lambda i: (0, 0))],
        out_shape=[
            jax.ShapeDtypeStruct((3, npoint), jnp.float32),
            jax.ShapeDtypeStruct((ndevice, 2 * capacity), jnp.float32),
        ],
        scratch_shapes=[pltpu.VMEM((ndevice, 1), jnp.float32)],
        cost_estimate=pl.CostEstimate(
            flops=2 * npoint * capacity * 6 * ndevice, bytes_accessed=40000000, transcendentals=0
        ),
    )(
        padded, normals, tension[None], edge_weight, relative, owner_ids[None], cell_map[None]
    )


def scatter_kernel(rhs_ref, val_ref, row_ref, col_ref, out_ref):
    @pl.when(pl.program_id(0) == 0)
    def _():
        out_ref[...] = rhs_ref[...]

    nrow, ncol = out_ref.shape
    count = val_ref.shape[2]
    value = val_ref[0]
    first = value.astype(jnp.bfloat16)
    second = (value - first.astype(jnp.float32)).astype(jnp.bfloat16)
    by_row = (
        (lax.broadcasted_iota(jnp.int32, (nrow, count), 0) == row_ref[0])
        .astype(jnp.float32)
        .astype(jnp.bfloat16)
    )
    same = lax.broadcasted_iota(jnp.int32, (ncol, count), 0) == col_ref[0]
    total = out_ref[...]
    for piece in (first, second):
        by_col = jnp.where(same, piece.astype(jnp.float32), 0.0).astype(jnp.bfloat16)
        total = total + lax.dot_general(
            by_row, by_col, (((1,), (1,)), ((), ())), preferred_element_type=jnp.float32
        )
    out_ref[...] = total


def scatter(rhs, values, cells):
    nx, ny, nz = rhs.shape
    nrow = nx * ny
    sources, count = values.shape
    rows = cells // nz
    cols = cells - rows * nz
    one = pl.BlockSpec((1, 1, count), lambda i: (i, 0, 0))
    whole = pl.BlockSpec((nrow, nz), lambda i: (0, 0))
    out = pl.pallas_call(
        scatter_kernel,
        grid=(sources,),
        in_specs=[whole, one, one, one],
        out_specs=whole,
        out_shape=jax.ShapeDtypeStruct((nrow, nz), jnp.float32),
        cost_estimate=pl.CostEstimate(
            flops=4 * nrow * nz * sources * count, bytes_accessed=4000000, transcendentals=0
        ),
    )(rhs.reshape(nrow, nz), values[:, None], rows[:, None], cols[:, None])
    return out.reshape(nx, ny, nz)


def body(
    pressure_rhs,
    shift_diag,
    positions,
    normals,
    tension,
    edge_weight,
    owner_map,
    cell_map,
    connectivity,
):
    npoint = positions.shape[1]
    ndevice = lax.axis_size(("gx", "gy", "gz"))
    total = npoint * ndevice
    begin = lax.axis_index(("gx", "gy", "gz")) * npoint
    padded = padded_2(positions, ((("gx", "gy", "gz"), 1, HALO),), True)
    relative = (connectivity - begin + HALO + total) % total
    capacity = 4 * npoint // ndevice
    surface_force, packed = points(
        padded, normals, tension, edge_weight, relative, owner_map[:, 0], cell_map,
        ndevice, capacity,
    )
    got = lax.all_to_all(packed, ("gx", "gy", "gz"), split_axis=0, concat_axis=0, tiled=True)
    forcing = scatter(pressure_rhs, got[:, :capacity], got[:, capacity:].astype(jnp.int32))

    nx, ny, nz = pressure_rhs.shape
    wx, wy, wz = 2 * SMOOTH - 1, 8, 128
    cx = COARSE_SMOOTH - 1 + (SMOOTH + 1) // 2
    sides = (("gz", 2, wz), ("gy", 1, wy), ("gx", 0, wx))
    coarse_sides = (("gz", 3, wz), ("gy", 2, wy), ("gx", 1, cx))
    coarse_shift = 0.5 * pool(shift_diag)
    inverse = padded_2(1.0 / (6.0 + shift_diag), sides, False)
    rhs = padded_2(forcing, sides, False)
    wide = jax.ShapeDtypeStruct(rhs.shape, jnp.float32)
    core = jax.ShapeDtypeStruct(pressure_rhs.shape, jnp.float32)
    vmem = pl.BlockSpec(memory_space=pltpu.VMEM)
    wide_buf = pltpu.VMEM(rhs.shape, jnp.float32)
    smooth, remain = pl.pallas_call(
        functools.partial(down_kernel, wx, wy, wz),
        in_specs=[vmem] * 3,
        out_specs=[vmem] * 2,
        out_shape=[wide, core],
        scratch_shapes=[wide_buf] * 2,
    )(rhs, inverse, shift_diag)
    coarse = padded_2(
        jnp.stack([0.5 * pool(remain), 1.0 / (6.0 + coarse_shift)]), coarse_sides, False
    )
    fix_buf = pltpu.VMEM(coarse.shape[1:], jnp.float32)
    pressure = pl.pallas_call(
        functools.partial(up_kernel, wx, wy, wz, cx),
        in_specs=[vmem] * 4,
        out_specs=vmem,
        out_shape=core,
        scratch_shapes=[fix_buf] * 3 + [wide_buf] * 3,
    )(coarse, rhs, inverse, smooth)
    return (pressure, surface_force)


def solution(mesh):
    return jax.shard_map(
        body,
        mesh=mesh,
        in_specs=(
            P("gx", "gy", "gz"),
            P("gx", "gy", "gz"),
            P(None, ("gx", "gy", "gz")),
            P(None, ("gx", "gy", "gz")),
            P(("gx", "gy", "gz")),
            P(None, ("gx", "gy", "gz")),
            P(("gx", "gy", "gz"), None),
            P(("gx", "gy", "gz")),
            P(None, ("gx", "gy", "gz")),
        ),
        out_specs=(P("gx", "gy", "gz"), P(None, ("gx", "gy", "gz"))),
        check_vma=False,
    )
```

```python
import functools

import jax
import jax.numpy as jnp
from jax import lax
from jax.experimental import pallas as pl
from jax.experimental.pallas import tpu as pltpu
from jax.sharding import PartitionSpec as P

HALO = 64
SMOOTH = 3
COARSE_SMOOTH = 4


centre = 1.125
spread = 0.875


def padded_2(cells, sides, closed):
    for axis, dim, width in sides:
        count = lax.axis_size(axis)
        ends = count if closed else count - 1
        head = lax.slice_in_dim(cells, 0, width, axis=dim)
        tail = lax.slice_in_dim(cells, cells.shape[dim] - width, cells.shape[dim], axis=dim)
        cells = jnp.concatenate(
            [
                lax.ppermute(tail, axis, [(i, (i + 1) % count) for i in range(ends)]),
                cells,
                lax.ppermute(head, axis, [((i + 1) % count, i) for i in range(ends)]),
            ],
            axis=dim,
        )
    return cells


def factors(sweeps):
    ratio = centre / spread
    fac = 1.0 / ratio
    pairs = [(0.0, 1.0 / centre)]
    for _ in range(1, sweeps):
        fac_new = 1.0 / (2.0 * ratio - fac)
        pairs.append((fac_new * fac, 2.0 * fac_new / spread))
        fac = fac_new
    return pairs


def beside(ref, x, cells):
    ny, nz = cells.shape
    total = ref[x - 1] + ref[x + 1]
    total = total + pltpu.roll(cells, 1, 0) + pltpu.roll(cells, ny - 1, 0)
    return total + pltpu.roll(cells, 1, 1) + pltpu.roll(cells, nz - 1, 1)


def sweep(rhs, inverse, src, dst, update, first, last, pair, keep=None):
    old, new = pair

    def slab(x, carry):
        cells = src[x]
        change = new * (inverse[x] * (rhs[x] + beside(src, x, cells)) - cells)
        if old:
            change = change + old * update[x]
        if keep is None:
            update[x] = change
            dst[x] = cells + change
        else:
            keep(x, cells + change)
        return carry

    lax.fori_loop(first, last, slab, 0)


def begin(rhs, inverse, dst, update, slabs):
    def slab(x, carry):
        change = inverse[x] * rhs[x] * (1.0 / centre)
        update[x] = change
        dst[x] = change
        return carry

    lax.fori_loop(0, slabs, slab, 0)


def down_kernel(wx, wy, wz, rhs, inverse, shift, smooth, remain, one, update):
    slabs = rhs.shape[0]
    ny, nz = remain.shape[1:]
    pairs = factors(SMOOTH)
    bufs = (one, smooth) if SMOOTH % 2 == 0 else (smooth, one)
    begin(rhs, inverse, bufs[0], update, slabs)
    for k in range(1, SMOOTH):
        sweep(
            rhs, inverse, bufs[(k - 1) % 2], bufs[k % 2], update, k, slabs - k, pairs[k]
        )

    def slab(x, carry):
        cells = smooth[x]
        near = rhs[x] + beside(smooth, x, cells)
        core = (slice(wy, wy + ny), slice(wz, wz + nz))
        remain[x - wx] = near[core] - (6.0 + shift[x - wx]) * cells[core]
        return carry

    lax.fori_loop(wx, slabs - wx, slab, 0)


def up_kernel(
    wx, wy, wz, cx, coarse, rhs, inverse, smooth, pressure,
    fix_a, fix_b, fix_update, one, two, update,
):
    crhs, cinverse = coarse.at[0], coarse.at[1]
    cslabs, cny, cnz = fix_a.shape
    slabs, fny, fnz = one.shape
    ny, nz = pressure.shape[1:]
    pairs = factors(COARSE_SMOOTH)
    bufs = (fix_a, fix_b)
    begin(crhs, cinverse, fix_a, fix_update, cslabs)
    for k in range(1, COARSE_SMOOTH):
        sweep(
            crhs, cinverse, bufs[(k - 1) % 2], bufs[k % 2], fix_update, k, cslabs - k, pairs[k]
        )
    fix = bufs[(COARSE_SMOOTH - 1) % 2]

    low = cx - (SMOOTH + 1) // 2
    count = cslabs - 2 * low
    flat = fix[low : low + count].reshape(count * cny, cnz)

    def onehot(shape, offset_f, offset_c, fine_dim, fine_per, coarse_per):
        f = lax.broadcasted_iota(jnp.int32, shape, fine_dim)
        c = lax.broadcasted_iota(jnp.int32, shape, 1 - fine_dim)
        block, inner = 0, f
        for g in range(1, shape[fine_dim] // fine_per):
            block = block + (f >= g * fine_per).astype(jnp.int32)
        inner = f - block * fine_per
        half = jnp.right_shift(inner - offset_f + 2 * offset_c, 1)
        return (c == half + block * coarse_per).astype(jnp.float32).astype(jnp.bfloat16)

    fan_y = onehot((count * fny, count * cny), wy, wy, 0, fny, cny)
    fan_z = onehot((cnz, fnz), wz, wz, 1, fnz, cnz)
    tall = sum(
        jnp.dot(fan_y, piece, preferred_element_type=jnp.float32) for piece in split3(flat)
    )
    full = sum(
        jnp.dot(piece, fan_z, preferred_element_type=jnp.float32) for piece in split3(tall)
    )
    for j in range(count):
        part = full[j * fny : (j + 1) * fny]
        for half in range(2):
            x = wx + 2 * (low + j - cx) + half
            if wx - SMOOTH <= x < slabs - wx + SMOOTH:
                one[x] = smooth[x] + part

    pairs = factors(SMOOTH)
    bufs = (one, two)

    def keep(x, cells):
        pressure[x - wx] = cells[wy : wy + ny, wz : wz + nz]

    edge = wx - SMOOTH
    for k in range(SMOOTH):
        sweep(
            rhs, inverse, bufs[k % 2], bufs[(k + 1) % 2], update,
            edge + k + 1, slabs - edge - k - 1, pairs[k], keep if k == SMOOTH - 1 else None,
        )


LANES = 2 * HALO
HIGH = lax.Precision.HIGHEST


def pair_matrix(rows, cols, offset=0):
    r = lax.broadcasted_iota(jnp.int32, (rows, cols), 0)
    c = lax.broadcasted_iota(jnp.int32, (rows, cols), 1)
    return (r == (c + offset) // 2).astype(jnp.float32)


def pool(field):
    nx, ny, nz = field.shape
    halves = jnp.sum(field.reshape(nx // 2, 2, ny, nz), axis=1)
    flat = halves.reshape(nx // 2 * ny, nz)
    along_z = jnp.dot(flat, pair_matrix(nz // 2, nz).T, precision=HIGH)
    along_y = jnp.dot(
        pair_matrix(nx // 2 * ny // 2, nx // 2 * ny), along_z, precision=HIGH
    )
    return along_y.reshape(nx // 2, ny // 2, nz // 2)


def split3(x):
    a = x.astype(jnp.bfloat16)
    rest = x - a.astype(jnp.float32)
    b = rest.astype(jnp.bfloat16)
    c = (rest - b.astype(jnp.float32)).astype(jnp.bfloat16)
    return a, b, c


def points_kernel(
    ndevice, capacity, pos_ref, nrm_ref, ten_ref, wgt_ref, con_ref, own_ref, cel_ref,
    force_ref, packed_ref, carry_ref,
):
    step = pl.program_id(0)
    chunk = ten_ref.shape[1]

    @pl.when(step == 0)
    def _():
        packed_ref[...] = jnp.zeros_like(packed_ref)
        carry_ref[...] = jnp.zeros_like(carry_ref)

    jumps = []
    for sub in range(chunk // LANES):
        here = pl.ds(sub * LANES, LANES)
        base = pl.multiple_of(step * chunk + sub * LANES, LANES)
        lower = pos_ref[:, pl.ds(base, LANES)]
        upper = pos_ref[:, pl.ds(base + LANES, LANES)]
        centre_pos = jnp.concatenate([lower[:, HALO:], upper[:, :HALO]], axis=1)
        total = jnp.zeros_like(lower)
        for which in range(con_ref.shape[0]):
            index = con_ref[which : which + 1, here] - base
            wide = jnp.broadcast_to(index, lower.shape)
            low = jnp.bitwise_and(wide, LANES - 1)
            near = jnp.take_along_axis(lower, low, axis=1, mode="promise_in_bounds")
            far = jnp.take_along_axis(upper, low, axis=1, mode="promise_in_bounds")
            picked = jnp.where(wide < LANES, near, far)
            total = total + wgt_ref[which : which + 1, here] * (picked - centre_pos)
        force = ten_ref[:, here] * total[:3]
        force_ref[:, here] = force
        jumps.append(jnp.sum(force * nrm_ref[:, here], axis=0, keepdims=True))
    jump = jnp.concatenate(jumps, axis=1)

    hot = (lax.broadcasted_iota(jnp.int32, (ndevice, chunk), 0) == own_ref[...]).astype(jnp.float32)
    hot_half = hot.astype(jnp.bfloat16)
    before = (
        lax.broadcasted_iota(jnp.int32, (chunk, chunk), 0)
        < lax.broadcasted_iota(jnp.int32, (chunk, chunk), 1)
    ).astype(jnp.bfloat16)
    earlier = jnp.dot(hot_half, before, preferred_element_type=jnp.float32) + carry_ref[...]
    rank = jnp.sum(hot * earlier, axis=0, keepdims=True).astype(jnp.int32)
    carry_ref[...] = carry_ref[...] + jnp.sum(hot, axis=1, keepdims=True)
    slots = (
        lax.broadcasted_iota(jnp.int32, (capacity, chunk), 0) == rank
    ).astype(jnp.float32).astype(jnp.bfloat16)
    cell = cel_ref[...]
    parts = [piece.astype(jnp.float32) for piece in split3(jump)]
    for bits in (0, 8, 16):
        piece = jnp.bitwise_and(jnp.right_shift(cell, bits), 255).astype(jnp.float32)
        parts.append(piece)
    left = jnp.concatenate([(hot * part).astype(jnp.bfloat16) for part in parts], axis=0)
    packed = lax.dot_general(
        left, slots, (((1,), (1,)), ((), ())), preferred_element_type=jnp.float32
    )
    n = ndevice
    values = packed[0:n] + packed[n : 2 * n] + packed[2 * n : 3 * n]
    cells = packed[3 * n : 4 * n] + 256.0 * packed[4 * n : 5 * n] + 65536.0 * packed[5 * n :]
    packed_ref[:, :capacity] += values
    packed_ref[:, capacity:] += cells


def points(padded, normals, tension, edge_weight, relative, owner_ids, cell_map, ndevice, capacity):
    npoint = tension.shape[0]
    chunk = 4 * LANES if npoint % (4 * LANES) == 0 else LANES
    padded = jnp.concatenate([padded, jnp.zeros((5, padded.shape[1]), jnp.float32)], axis=0)
    neigh = relative.shape[0]

    def rows(count):
        return pl.BlockSpec((count, chunk), lambda i: (0, i))

    return pl.pallas_call(
        functools.partial(points_kernel, ndevice, capacity),
        grid=(npoint // chunk,),
        in_specs=[
            pl.BlockSpec(padded.shape, lambda i: (0, 0)),
            rows(3), rows(1), rows(neigh), rows(neigh), rows(1), rows(1),
        ],
        out_specs=[rows(3), pl.BlockSpec((ndevice, 2 * capacity), lambda i: (0, 0))],
        out_shape=[
            jax.ShapeDtypeStruct((3, npoint), jnp.float32),
            jax.ShapeDtypeStruct((ndevice, 2 * capacity), jnp.float32),
        ],
        scratch_shapes=[pltpu.VMEM((ndevice, 1), jnp.float32)],
        cost_estimate=pl.CostEstimate(
            flops=2 * npoint * capacity * 6 * ndevice, bytes_accessed=40000000, transcendentals=0
        ),
    )(
        padded, normals, tension[None], edge_weight, relative, owner_ids[None], cell_map[None]
    )


def scatter_kernel(rhs_ref, val_ref, row_ref, col_ref, out_ref):
    @pl.when(pl.program_id(0) == 0)
    def _():
        out_ref[...] = rhs_ref[...]

    nrow, ncol = out_ref.shape
    count = val_ref.shape[2]
    value = val_ref[0]
    first = value.astype(jnp.bfloat16)
    second = (value - first.astype(jnp.float32)).astype(jnp.bfloat16)
    by_row = (
        (lax.broadcasted_iota(jnp.int32, (nrow, count), 0) == row_ref[0])
        .astype(jnp.float32)
        .astype(jnp.bfloat16)
    )
    same = lax.broadcasted_iota(jnp.int32, (ncol, count), 0) == col_ref[0]
    total = out_ref[...]
    for piece in (first, second):
        by_col = jnp.where(same, piece.astype(jnp.float32), 0.0).astype(jnp.bfloat16)
        total = total + lax.dot_general(
            by_row, by_col, (((1,), (1,)), ((), ())), preferred_element_type=jnp.float32
        )
    out_ref[...] = total


def scatter(rhs, values, cells):
    nx, ny, nz = rhs.shape
    nrow = nx * ny
    sources, count = values.shape
    rows = cells // nz
    cols = cells - rows * nz
    one = pl.BlockSpec((1, 1, count), lambda i: (i, 0, 0))
    whole = pl.BlockSpec((nrow, nz), lambda i: (0, 0))
    out = pl.pallas_call(
        scatter_kernel,
        grid=(sources,),
        in_specs=[whole, one, one, one],
        out_specs=whole,
        out_shape=jax.ShapeDtypeStruct((nrow, nz), jnp.float32),
        cost_estimate=pl.CostEstimate(
            flops=4 * nrow * nz * sources * count, bytes_accessed=4000000, transcendentals=0
        ),
    )(rhs.reshape(nrow, nz), values[:, None], rows[:, None], cols[:, None])
    return out.reshape(nx, ny, nz)


def body(
    pressure_rhs,
    shift_diag,
    positions,
    normals,
    tension,
    edge_weight,
    owner_map,
    cell_map,
    connectivity,
):
    npoint = positions.shape[1]
    ndevice = lax.axis_size(("gx", "gy", "gz"))
    total = npoint * ndevice
    begin = lax.axis_index(("gx", "gy", "gz")) * npoint
    padded = padded_2(positions, ((("gx", "gy", "gz"), 1, HALO),), True)
    relative = (connectivity - begin + HALO + total) % total
    capacity = 4 * npoint // ndevice
    surface_force, packed = points(
        padded, normals, tension, edge_weight, relative, owner_map[:, 0], cell_map,
        ndevice, capacity,
    )
    wx, wy, wz = 2 * SMOOTH - 1, 8, 128
    sides = (("gz", 2, wz), ("gy", 1, wy), ("gx", 0, wx))
    inverse = padded_2(1.0 / (6.0 + shift_diag), sides[:1], False)
    packed, inverse = lax.optimization_barrier((packed, inverse))
    inverse = padded_2(inverse, sides[1:2], False)
    got = lax.all_to_all(packed, ("gx", "gy", "gz"), split_axis=0, concat_axis=0, tiled=True)
    got, inverse = lax.optimization_barrier((got, inverse))
    inverse = padded_2(inverse, sides[2:], False)
    forcing = scatter(pressure_rhs, got[:, :capacity], got[:, capacity:].astype(jnp.int32))

    nx, ny, nz = pressure_rhs.shape
    cx = COARSE_SMOOTH - 1 + (SMOOTH + 1) // 2
    coarse_sides = (("gz", 3, wz), ("gy", 2, wy), ("gx", 1, cx))
    coarse_shift = 0.5 * pool(shift_diag)
    forcing, inverse = lax.optimization_barrier((forcing, inverse))
    rhs = padded_2(forcing, sides, False)
    wide = jax.ShapeDtypeStruct(rhs.shape, jnp.float32)
    core = jax.ShapeDtypeStruct(pressure_rhs.shape, jnp.float32)
    vmem = pl.BlockSpec(memory_space=pltpu.VMEM)
    wide_buf = pltpu.VMEM(rhs.shape, jnp.float32)
    smooth, remain = pl.pallas_call(
        functools.partial(down_kernel, wx, wy, wz),
        in_specs=[vmem] * 3,
        out_specs=[vmem] * 2,
        out_shape=[wide, core],
        scratch_shapes=[wide_buf] * 2,
    )(rhs, inverse, shift_diag)
    coarse = padded_2(
        jnp.stack([0.5 * pool(remain), 1.0 / (6.0 + coarse_shift)]), coarse_sides, False
    )
    fix_buf = pltpu.VMEM(coarse.shape[1:], jnp.float32)
    pressure = pl.pallas_call(
        functools.partial(up_kernel, wx, wy, wz, cx),
        in_specs=[vmem] * 4,
        out_specs=vmem,
        out_shape=core,
        scratch_shapes=[fix_buf] * 3 + [wide_buf] * 3,
    )(coarse, rhs, inverse, smooth)
    return (pressure, surface_force)


def solution(mesh):
    return jax.shard_map(
        body,
        mesh=mesh,
        in_specs=(
            P("gx", "gy", "gz"),
            P("gx", "gy", "gz"),
            P(None, ("gx", "gy", "gz")),
            P(None, ("gx", "gy", "gz")),
            P(("gx", "gy", "gz")),
            P(None, ("gx", "gy", "gz")),
            P(("gx", "gy", "gz"), None),
            P(("gx", "gy", "gz")),
            P(None, ("gx", "gy", "gz")),
        ),
        out_specs=(P("gx", "gy", "gz"), P(None, ("gx", "gy", "gz"))),
        check_vma=False,
    )
```
